32 devices in a mesh: dp: 1 (over z), tp: 4 (over y), ep: 8 (over x, core).
Axes of the slice: x: 4, y: 4, z: 1, core: 2. Of those that a mesh axis runs over, the one named last changes fastest.
The devices are a block of a 4x4x8 slice.
Arguments:
- tokens: bfloat16 [32768, 768], P(('dp', 'ep', 'tp'))
- route_ids: int32 [32768, 2], P(('dp', 'ep', 'tp'))
- w_router: bfloat16 [768, 16], replicated
- w_gate: bfloat16 [16, 768, 3072], P('ep', None, 'tp')
- w_up: bfloat16 [16, 768, 3072], P('ep', None, 'tp')
- w_down: bfloat16 [16, 3072, 768], P('ep', 'tp')
- d_out: bfloat16 [32768, 768], P(('dp', 'ep', 'tp'))
Outputs:
- output 1: bfloat16 [32768, 768], P(('dp', 'ep', 'tp'))
- output 2: bfloat16 [32768, 768], P(('dp', 'ep', 'tp'))
- output 3: bfloat16 [16, 768, 3072], P(('dp', 'ep'), None, 'tp')
- output 4: bfloat16 [16, 768, 3072], P(('dp', 'ep'), None, 'tp')
- output 5: bfloat16 [16, 3072, 768], P(('dp', 'ep'), 'tp')
- output 6: float32 [768, 16], P('dp')
All inputs are finite; a program needn't handle non-finite values.
Results may differ from the reference program's by a relative error of at most 0.0124595.
Values are sent between devices in bfloat16 or wider.
A program may use at most 768 MiB of HBM per device.

```python
import math
import jax
import jax.numpy as jnp
from jax import lax

D = 768
FF = 3072
EXPERTS = 16
TOK = 1024
EP_SIZE = 8
TP_SIZE = 4

SHARDS = EP_SIZE * TP_SIZE
TOKEN_ROWS = SHARDS * TOK
CAPACITY = 4 * TOK // EXPERTS
HOT_COUNT = 4 * TOK // EXPERTS + TOK // 8
F_SHARD = FF // TP_SIZE


def draw_route(rng_key):
    k_perm, k_base, k_hot, k_rank, k_shift = jax.random.split(rng_key, 5)
    cover_ids = jax.random.permutation(k_perm, EXPERTS)
    base_ids = jax.random.randint(k_base, (TOK - EXPERTS,), 0, EXPERTS)
    hot_id = jax.random.randint(k_hot, (), 0, EXPERTS)
    rank_perm = jax.random.permutation(k_rank, TOK - EXPERTS)
    first_ids = jnp.concatenate([cover_ids, jnp.where(rank_perm < HOT_COUNT, hot_id, base_ids)])
    shift_ids = jax.random.randint(k_shift, (TOK,), 1, EXPERTS)
    second_ids = (first_ids + shift_ids) % EXPERTS
    return jnp.stack([first_ids, second_ids], axis=1).astype(jnp.int32)


def setup_inputs(seed: int = 0, part: int = 0) -> dict:
    root_key = jax.random.key(seed)
    part_key = jax.random.fold_in(root_key, part)
    k_tok, k_ids, k_dy = jax.random.split(part_key, 3)
    shared_key = jax.random.key(seed + 1)
    k_router, k_gate, k_up, k_down = jax.random.split(shared_key, 4)
    tokens = jax.random.normal(k_tok, (TOKEN_ROWS, D), jnp.float32).astype(jnp.bfloat16)
    route_ids = jax.vmap(draw_route)(jax.random.split(k_ids, SHARDS)).reshape(TOKEN_ROWS, 2)
    w_router = (jax.random.normal(k_router, (D, EXPERTS), jnp.float32) / math.sqrt(D)).astype(jnp.bfloat16)
    w_gate = (jax.random.normal(k_gate, (EXPERTS, D, FF), jnp.float32) / math.sqrt(D)).astype(jnp.bfloat16)
    w_up = (jax.random.normal(k_up, (EXPERTS, D, FF), jnp.float32) / math.sqrt(D)).astype(jnp.bfloat16)
    w_down = (jax.random.normal(k_down, (EXPERTS, FF, D), jnp.float32) / math.sqrt(FF)).astype(jnp.bfloat16)
    d_out = jax.random.normal(k_dy, (TOKEN_ROWS, D), jnp.float32).astype(jnp.bfloat16)
    return dict(tokens=tokens, route_ids=route_ids, w_router=w_router, w_gate=w_gate, w_up=w_up, w_down=w_down, d_out=d_out)


def route_shard(x_block, ids_block, w_router):
    expert_ids = jnp.arange(EXPERTS)
    logits = jnp.dot(x_block, w_router, preferred_element_type=jnp.float32)
    choice_hot = (ids_block[:, :, None] == expert_ids[None, None, :]).astype(jnp.float32)
    chosen = jnp.einsum('te,tke->tk', logits, choice_hot)
    gate_vals = jax.nn.softmax(chosen, axis=1)
    slot_order = (ids_block.T[:, :, None] == expert_ids).astype(jnp.int32).reshape(2 * TOK, EXPERTS)
    before = jnp.cumsum(slot_order, axis=0) - slot_order
    slot_pos = jnp.sum(before * slot_order, axis=1).reshape(2, TOK).T
    slot_hot = (slot_pos[:, :, None] == jnp.arange(CAPACITY)).astype(jnp.float32)
    select = choice_hot[:, :, :, None] * slot_hot[:, :, None, :]
    return gate_vals, choice_hot, select


def reference(tokens, route_ids, w_router, w_gate, w_up, w_down, d_out):
    x_blocks = tokens.reshape(SHARDS, TOK, D)
    id_blocks = route_ids.reshape(SHARDS, TOK, 2)
    dy_blocks = d_out.reshape(SHARDS, TOK, D)

    def dispatch(operands):
        x_one, ids_one, dy_one = operands
        gate_vals, choice_hot, select = route_shard(x_one, ids_one, w_router)
        x_rows = jnp.einsum('tkec,td->ecd', select, x_one.astype(jnp.float32)).astype(jnp.bfloat16)
        grad_slot = (gate_vals[:, :, None] * dy_one.astype(jnp.float32)[:, None, :]).astype(jnp.bfloat16)
        grad_rows = jnp.einsum('tkec,tkd->ecd', select, grad_slot.astype(jnp.float32)).astype(jnp.bfloat16)
        return x_rows, grad_rows

    x_rows, grad_rows = lax.map(dispatch, (x_blocks, id_blocks, dy_blocks))
    x_rows = x_rows.transpose(1, 0, 2, 3).reshape(EXPERTS, SHARDS * CAPACITY, D)
    grad_rows = grad_rows.transpose(1, 0, 2, 3).reshape(EXPERTS, SHARDS * CAPACITY, D)

    def expert(operands):
        x_in, grad_in, w_one, w_three, w_two = operands
        h_gate = jnp.dot(x_in, w_one, preferred_element_type=jnp.float32)
        h_up = jnp.dot(x_in, w_three, preferred_element_type=jnp.float32)
        hidden_act = (jax.nn.silu(h_gate) * h_up).astype(jnp.bfloat16)
        act_split = hidden_act.reshape(-1, TP_SIZE, F_SHARD).astype(jnp.float32)
        down_split = w_two.reshape(TP_SIZE, F_SHARD, D).astype(jnp.float32)
        out_parts = jnp.einsum('rjf,jfd->jrd', act_split, down_split).astype(jnp.bfloat16)
        expert_out = jnp.sum(out_parts.astype(jnp.float32), axis=0).astype(jnp.bfloat16)
        d_act = jnp.dot(grad_in, w_two.T, preferred_element_type=jnp.float32)
        gate_sig = jax.nn.sigmoid(h_gate)
        dz_up = (d_act * h_gate * gate_sig).astype(jnp.bfloat16)
        dz_gate = (d_act * h_up * gate_sig * (1.0 + h_gate * (1.0 - gate_sig))).astype(jnp.bfloat16)
        g_gate = jnp.dot(x_in.T, dz_gate, preferred_element_type=jnp.float32).astype(jnp.bfloat16)
        g_up = jnp.dot(x_in.T, dz_up, preferred_element_type=jnp.float32).astype(jnp.bfloat16)
        g_down = jnp.dot(hidden_act.T, grad_in, preferred_element_type=jnp.float32).astype(jnp.bfloat16)
        gate_parts = jnp.einsum('rjf,djf->jrd', dz_gate.reshape(-1, TP_SIZE, F_SHARD).astype(jnp.float32), w_one.reshape(D, TP_SIZE, F_SHARD).astype(jnp.float32))
        up_parts = jnp.einsum('rjf,djf->jrd', dz_up.reshape(-1, TP_SIZE, F_SHARD).astype(jnp.float32), w_three.reshape(D, TP_SIZE, F_SHARD).astype(jnp.float32))
        back_parts = (gate_parts + up_parts).astype(jnp.bfloat16)
        expert_dx = jnp.sum(back_parts.astype(jnp.float32), axis=0).astype(jnp.bfloat16)
        return expert_out, expert_dx, g_gate, g_up, g_down

    expert_out, expert_dx, grad_gate, grad_up, grad_down = lax.map(expert, (x_rows, grad_rows, w_gate, w_up, w_down))
    expert_out = expert_out.reshape(EXPERTS, SHARDS, CAPACITY, D).transpose(1, 0, 2, 3)
    expert_dx = expert_dx.reshape(EXPERTS, SHARDS, CAPACITY, D).transpose(1, 0, 2, 3)

    def combine(operands):
        x_one, ids_one, dy_one, out_one, dx_one = operands
        gate_vals, choice_hot, select = route_shard(x_one, ids_one, w_router)
        picked = jnp.einsum('tkec,ecd->tkd', select, out_one.astype(jnp.float32))
        block_out = jnp.sum(gate_vals[:, :, None] * picked, axis=1).astype(jnp.bfloat16)
        d_gates = jnp.einsum('tkd,td->tk', picked, dy_one.astype(jnp.float32))
        d_chosen = gate_vals * (d_gates - jnp.sum(gate_vals * d_gates, axis=1, keepdims=True))
        d_logits = jnp.einsum('tk,tke->te', d_chosen, choice_hot).astype(jnp.bfloat16)
        router_part = jnp.dot(x_one.T, d_logits, preferred_element_type=jnp.float32)
        from_experts = jnp.einsum('tkec,ecd->td', select, dx_one.astype(jnp.float32))
        grad_x = (from_experts + jnp.dot(d_logits, w_router.T, preferred_element_type=jnp.float32)).astype(jnp.bfloat16)
        return block_out, grad_x, router_part

    block_out, grad_x, router_part = lax.map(combine, (x_blocks, id_blocks, dy_blocks, expert_out, expert_dx))
    return (block_out.reshape(TOKEN_ROWS, D), grad_x.reshape(TOKEN_ROWS, D), grad_gate, grad_up, grad_down, jnp.sum(router_part, axis=0))
```

```python
import functools
import jax
import jax.numpy as jnp
from jax import lax
from jax.experimental import pallas as pl
from jax.experimental.pallas import tpu as pltpu
from jax.sharding import PartitionSpec as P

F32 = jnp.float32
BF16 = jnp.bfloat16
KEY_STRIDE = 4096
BLOCKS_PER_STEP = 2


def nn(a, b):
    return lax.dot_general(a, b, (((1,), (0,)), ((), ())), preferred_element_type=F32)


def nt(a, b):
    return lax.dot_general(a, b, (((1,), (1,)), ((), ())), preferred_element_type=F32)


def tn(a, b):
    return lax.dot_general(a, b, (((0,), (0,)), ((), ())), preferred_element_type=F32)


def hidden(h1, h3):
    sig = jax.nn.sigmoid(h1)
    return sig, (h1 * sig * h3).astype(BF16)


def hidden_back(da, h1, h3, sig):
    das = da * sig
    dz3 = (das * h1).astype(BF16)
    dz1 = (das * h3 * (1.0 + h1 * (1.0 - sig))).astype(BF16)
    return dz1, dz3


def route_local(tokens, route_ids, w_router):
    experts = w_router.shape[1]
    tok_loc = tokens.shape[0]
    expert_ids = jnp.arange(experts)
    logits = jnp.dot(tokens, w_router, preferred_element_type=F32)
    choice_hot = (route_ids[:, :, None] == expert_ids).astype(F32)
    chosen = jnp.sum(logits[:, None, :] * choice_hot, axis=2)
    gate_vals = jax.nn.softmax(chosen, axis=1)
    slot_order = (route_ids.T[:, :, None] == expert_ids).astype(jnp.int32).reshape(2 * tok_loc, experts)
    before = jnp.cumsum(slot_order, axis=0) - slot_order
    slot_pos = jnp.sum(before * slot_order, axis=1).reshape(2, tok_loc).T
    return gate_vals, slot_pos


def wgrad_kernel(pos_ref, tok_ref, dy_ref, meta_ref, w1_ref, w3_ref, w2_ref,
                 dw1_ref, dw3_ref, dw2_ref, xo_ref, go_ref,
                 acc1, acc3, acc2, xs, gs, az, z1, z3):
    step = pl.program_id(0)
    e_loc, cap = xo_ref.shape[1], xo_ref.shape[2]
    tok_loc, width = tok_ref.shape[1], tok_ref.shape[2]
    cols = w1_ref.shape[2]
    chunk = 256

    @pl.when(step == 0)
    def _():
        acc1[...] = jnp.zeros_like(acc1)
        acc3[...] = jnp.zeros_like(acc3)
        acc2[...] = jnp.zeros_like(acc2)

    tp_size = pos_ref[2]
    slots = lax.broadcasted_iota(jnp.int32, (cap, tok_loc), 0).astype(F32)

    def per_expert(e, carry):
        base = ((pos_ref[0] * e_loc + e) * KEY_STRIDE).astype(F32)
        for b in range(BLOCKS_PER_STEP):
            k0 = meta_ref[b, 0:1, :] - base
            k1 = meta_ref[b, 1:2, :] - base
            use0 = jnp.logical_and(k0 >= 0.0, k0 < float(KEY_STRIDE))
            key = jnp.where(use0, k0, k1)
            gate = jnp.where(use0, meta_ref[b, 2:3, :], meta_ref[b, 3:4, :])
            hit = slots == key
            sel = jnp.where(hit, 1.0, 0.0).astype(BF16)
            g = jnp.sum(jnp.where(hit, gate, 0.0), axis=1, keepdims=True)
            rows = pl.ds(b * cap, cap)
            xs[e, rows, :] = nn(sel, tok_ref[b]).astype(BF16)
            gs[e, rows, :] = (nn(sel, dy_ref[b]) * g).astype(BF16)
        x = xs[e]
        dg = gs[e]
        for c in range(cols // chunk):
            cs = slice(c * chunk, (c + 1) * chunk)
            h1 = nn(x, w1_ref[e, :, cs])
            h3 = nn(x, w3_ref[e, :, cs])
            da = nt(dg, w2_ref[e, cs, :])
            sig, act = hidden(h1, h3)
            dz1, dz3 = hidden_back(da, h1, h3, sig)
            az[:, cs] = act
            z1[:, cs] = dz1
            z3[:, cs] = dz3
        acc1[e] += tn(x, z1[...])
        acc3[e] += tn(x, z3[...])
        acc2[e] += tn(az[...], dg)
        return carry

    lax.fori_loop(0, e_loc, per_expert, 0)

    per_group = tp_size // BLOCKS_PER_STEP
    mine = pos_ref[1]

    @pl.when(lax.rem(step, per_group) == mine // BLOCKS_PER_STEP)
    def _():
        rows = pl.ds(pl.multiple_of(lax.rem(mine, BLOCKS_PER_STEP) * cap, cap), cap)
        xo_ref[0] = xs[:, rows, :]
        go_ref[0] = gs[:, rows, :]

    @pl.when(step == pl.num_programs(0) - 1)
    def _():
        dw1_ref[...] = acc1[...].astype(BF16)
        dw3_ref[...] = acc3[...].astype(BF16)
        dw2_ref[...] = acc2[...].astype(BF16)


def weight_grads(pos, tok_all, dy_all, meta_all, w1, w3, w2, cap, tp_size):
    blocks, tok_loc, width = tok_all.shape
    e_loc, _, cols = w1.shape
    steps = blocks // BLOCKS_PER_STEP
    per_group = tp_size // BLOCKS_PER_STEP
    rows = BLOCKS_PER_STEP * cap
    whole = lambda shape: pl.BlockSpec(shape, lambda i, p: (0,) * len(shape))
    own = pl.BlockSpec((1, e_loc, cap, width), lambda i, p: (i // per_group, 0, 0, 0))
    grid_spec = pltpu.PrefetchScalarGridSpec(
        num_scalar_prefetch=1,
        grid=(steps,),
        in_specs=[
            pl.BlockSpec((BLOCKS_PER_STEP, tok_loc, width), lambda i, p: (i, 0, 0)),
            pl.BlockSpec((BLOCKS_PER_STEP, tok_loc, width), lambda i, p: (i, 0, 0)),
            pl.BlockSpec((BLOCKS_PER_STEP, meta_all.shape[1], tok_loc), lambda i, p: (i, 0, 0)),
            whole(w1.shape), whole(w3.shape), whole(w2.shape),
        ],
        out_specs=[whole(w1.shape), whole(w3.shape), whole(w2.shape), own, own],
        scratch_shapes=[
            pltpu.VMEM(w1.shape, F32), pltpu.VMEM(w3.shape, F32), pltpu.VMEM(w2.shape, F32),
            pltpu.VMEM((e_loc, rows, width), BF16), pltpu.VMEM((e_loc, rows, width), BF16),
            pltpu.VMEM((rows, cols), BF16), pltpu.VMEM((rows, cols), BF16), pltpu.VMEM((rows, cols), BF16),
        ],
    )
    own_shape = jax.ShapeDtypeStruct((blocks // tp_size, e_loc, cap, width), BF16)
    flops = 2 * blocks * e_loc * cap * (6 * width * cols + 2 * tok_loc * width)
    return pl.pallas_call(
        wgrad_kernel,
        grid_spec=grid_spec,
        out_shape=[jax.ShapeDtypeStruct(w.shape, BF16) for w in (w1, w3, w2)] + [own_shape, own_shape],
        compiler_params=pltpu.CompilerParams(dimension_semantics=("arbitrary",), vmem_limit_bytes=62 * 1024 * 1024),
        cost_estimate=pl.CostEstimate(flops=flops, bytes_accessed=4 * tok_all.size, transcendentals=0),
        name="weight_grads",
    )(pos, tok_all, dy_all, meta_all, w1, w3, w2)


def ep_peers(ep_size, me):
    return [lax.rem(me + k, ep_size) for k in range(1, ep_size)]


def rows_kernel(ep_size, tile, x_ref, g_ref, w_ref, home_ref, o_acc, q_acc, send, send_sem, recv_sem, self_sem):
    step = pl.program_id(0)
    steps = ep_size // tile
    me = lax.axis_index('ep')
    cap, width = x_ref.shape[2], x_ref.shape[3]

    @pl.when(step == 0)
    def _():
        barrier = pltpu.get_barrier_semaphore()
        for peer in ep_peers(ep_size, me):
            pl.semaphore_signal(barrier, inc=1, device_id={'ep': peer}, device_id_type=pl.DeviceIdType.MESH)
        pl.semaphore_wait(barrier, ep_size - 1)

    def first_of(at):
        return lax.rem(me // tile + at + 1, steps) * tile

    def remote(slot, dest):
        return pltpu.make_async_remote_copy(
            src_ref=send.at[slot], dst_ref=home_ref.at[me],
            send_sem=send_sem.at[slot], recv_sem=recv_sem.at[me],
            device_id={'ep': dest}, device_id_type=pl.DeviceIdType.MESH)

    @pl.when(step > 0)
    def _():
        for c in range(tile):
            remote((step - 1) * tile + c, first_of(step - 1) + c).start()

    dest = first_of(step)
    x = x_ref[pl.ds(dest, tile), 0].reshape(tile * cap, width)
    dg = g_ref[pl.ds(dest, tile), 0].reshape(tile * cap, width)
    o_acc[...] = jnp.zeros_like(o_acc)
    q_acc[...] = jnp.zeros_like(q_acc)

    def part(j, carry):
        w1 = w_ref[j, 0]
        w3 = w_ref[j, 1]
        w2 = w_ref[j, 2]
        h1 = nn(x, w1)
        h3 = nn(x, w3)
        da = nt(dg, w2)
        sig, act = hidden(h1, h3)
        dz1, dz3 = hidden_back(da, h1, h3, sig)
        o_acc[...] += nn(act, w2).astype(BF16).astype(F32)
        q_acc[...] += (nt(dz1, w1) + nt(dz3, w3)).astype(BF16).astype(F32)
        return carry

    lax.fori_loop(0, w_ref.shape[0], part, 0)
    for c in range(tile):
        rows = slice(c * cap, (c + 1) * cap)
        send[step * tile + c, 0] = o_acc[rows].astype(BF16)
        send[step * tile + c, 1] = q_acc[rows].astype(BF16)

    @pl.when(step == steps - 1)
    def _():
        last = (steps - 1) * tile
        mine = lax.rem(me, tile)
        own = pltpu.make_async_copy(send.at[last + mine], home_ref.at[me], self_sem)
        own.start()
        near = (me // tile) * tile
        for k in range(1, tile):
            c = lax.rem(mine + k, tile)
            remote(last + c, near + c).start()
        for slot in range(last):
            remote(slot, me).wait_send()
        for k in range(1, tile):
            remote(last + lax.rem(mine + k, tile), me).wait_send()
        for peer in ep_peers(ep_size, me):
            pltpu.make_async_remote_copy(
                src_ref=send.at[0], dst_ref=home_ref.at[peer],
                send_sem=send_sem.at[0], recv_sem=recv_sem.at[peer],
                device_id={'ep': peer}, device_id_type=pl.DeviceIdType.MESH).wait_recv()
        own.wait()


def own_rows(xo, go, wg, e, ep_size):
    groups, e_loc, cap, width = xo.shape
    tp_size, _, _, cols = wg.shape
    tile = 2
    in_rows = pl.BlockSpec((groups, 1, cap, width), lambda r: (0, e, 0, 0))
    flops = 12 * groups * cap * width * cols * tp_size
    return pl.pallas_call(
        functools.partial(rows_kernel, ep_size, tile),
        grid=(groups // tile,),
        in_specs=[in_rows, in_rows, pl.BlockSpec(wg.shape, lambda r: (0, 0, 0, 0))],
        out_specs=pl.BlockSpec(memory_space=pl.ANY),
        out_shape=jax.ShapeDtypeStruct((groups, 2, cap, width), BF16),
        scratch_shapes=[
            pltpu.VMEM((tile * cap, width), F32), pltpu.VMEM((tile * cap, width), F32),
            pltpu.VMEM((groups, 2, cap, width), BF16),
            pltpu.SemaphoreType.DMA((groups,)), pltpu.SemaphoreType.DMA((groups,)), pltpu.SemaphoreType.DMA,
        ],
        compiler_params=pltpu.CompilerParams(dimension_semantics=("arbitrary",), vmem_limit_bytes=62 * 1024 * 1024,
                                             collective_id=1 + e, has_side_effects=True),
        cost_estimate=pl.CostEstimate(flops=flops, bytes_accessed=4 * xo.size + 2 * wg.size, transcendentals=0),
        name="own_rows",
    )(xo, go, wg)


def combine_kernel(home0_ref, home1_ref, col_ref, tok_ref, dy_ref, wr_ref, y_ref, du_ref, dwr_ref, p0, p1, px):
    step = pl.program_id(0)
    cap = home0_ref.shape[2]
    tok_loc = tok_ref.shape[0]
    experts = wr_ref.shape[0]

    lane = lax.broadcasted_iota(jnp.int32, (1, 2 * cap), 1)
    target = (step * 2 * KEY_STRIDE + jnp.where(lane >= cap, lane + (KEY_STRIDE - cap), lane)).astype(F32)
    hit0 = col_ref[:, 0:1] == target
    hit1 = col_ref[:, 1:2] == target
    s0 = jnp.where(hit0, 1.0, 0.0).astype(BF16)
    s1 = jnp.where(hit1, 1.0, 0.0).astype(BF16)
    rows_o = jnp.concatenate([home0_ref[0, 0], home1_ref[0, 0]], axis=0)
    rows_x = jnp.concatenate([home0_ref[0, 1], home1_ref[0, 1]], axis=0)

    @pl.when(step == 0)
    def _():
        p0[...] = nn(s0, rows_o)
        p1[...] = nn(s1, rows_o)
        px[...] = nn(s0 + s1, rows_x)

    @pl.when(step > 0)
    def _():
        p0[...] += nn(s0, rows_o)
        p1[...] += nn(s1, rows_o)
        px[...] += nn(s0 + s1, rows_x)

    @pl.when(step == pl.num_programs(0) - 1)
    def _():
        g0 = col_ref[:, 2:3]
        g1 = col_ref[:, 3:4]
        dy = dy_ref[...].astype(F32)
        a0 = p0[...]
        a1 = p1[...]
        y_ref[...] = (g0 * a0 + g1 * a1).astype(BF16)
        d0 = jnp.sum(a0 * dy, axis=1, keepdims=True)
        d1 = jnp.sum(a1 * dy, axis=1, keepdims=True)
        mean = g0 * d0 + g1 * d1
        ids = lax.broadcasted_iota(jnp.int32, (tok_loc, experts), 1).astype(F32)
        dlog = (jnp.where(col_ref[:, 4:5] == ids, g0 * (d0 - mean), 0.0)
                + jnp.where(col_ref[:, 5:6] == ids, g1 * (d1 - mean), 0.0)).astype(BF16)
        du_ref[...] = (px[...] + nn(dlog, wr_ref[...])).astype(BF16)
        dwr_ref[...] = tn(dlog, tok_ref[...])


def combine(home0, home1, cols, tokens, d_out, wr_t):
    groups, _, cap, width = home0.shape
    tok_loc = tokens.shape[0]
    experts = wr_t.shape[0]
    home = pl.BlockSpec((1, 2, cap, width), lambda s: (s, 0, 0, 0))
    whole = lambda a: pl.BlockSpec(a.shape, lambda s: (0,) * a.ndim)
    return pl.pallas_call(
        combine_kernel,
        grid=(groups,),
        in_specs=[home, home, whole(cols), whole(tokens), whole(d_out), whole(wr_t)],
        out_specs=[whole(tokens), whole(tokens), pl.BlockSpec((experts, width), lambda s: (0, 0))],
        out_shape=[jax.ShapeDtypeStruct(tokens.shape, BF16), jax.ShapeDtypeStruct(tokens.shape, BF16),
                   jax.ShapeDtypeStruct((experts, width), F32)],
        scratch_shapes=[pltpu.VMEM(tokens.shape, F32)] * 3,
        compiler_params=pltpu.CompilerParams(dimension_semantics=("arbitrary",), vmem_limit_bytes=62 * 1024 * 1024),
        cost_estimate=pl.CostEstimate(flops=6 * tok_loc * experts * cap * width, bytes_accessed=4 * home0.size, transcendentals=0),
        name="combine",
    )(home0, home1, cols, tokens, d_out, wr_t)


def router_kernel(axes, part_ref, out_ref, buf_a, mid, buf_b, send_a, recv_a, send_b, recv_b):
    sizes = [size for _, size in axes]
    barrier = pltpu.get_barrier_semaphore()
    for name, size in axes:
        me = lax.axis_index(name)
        for k in range(1, size):
            pl.semaphore_signal(barrier, inc=1, device_id={name: lax.rem(me + k, size)}, device_id_type=pl.DeviceIdType.MESH)
    pl.semaphore_wait(barrier, sum(sizes) - len(sizes))

    def exchange(name, size, src, buf, send_sem, recv_sem, out):
        me = lax.axis_index(name)
        copies = []
        for k in range(1, size):
            copy = pltpu.make_async_remote_copy(
                src_ref=src, dst_ref=buf.at[me], send_sem=send_sem.at[k], recv_sem=recv_sem.at[me],
                device_id={name: lax.rem(me + k, size)}, device_id_type=pl.DeviceIdType.MESH)
            copy.start()
            copies.append(copy)
        buf[me] = src[...]
        for k in range(1, size):
            peer = lax.rem(me + k, size)
            pltpu.make_async_remote_copy(
                src_ref=src, dst_ref=buf.at[peer], send_sem=send_sem.at[k], recv_sem=recv_sem.at[peer],
                device_id={name: peer}, device_id_type=pl.DeviceIdType.MESH).wait_recv()
        total = buf[0]
        for k in range(1, size):
            total = total + buf[k]
        out[...] = total
        return copies

    copies = exchange(*axes[0], part_ref, buf_a, send_a, recv_a, mid)
    copies += exchange(*axes[1], mid, buf_b, send_b, recv_b, out_ref)
    for copy in copies:
        copy.wait_send()


def router_sum(part, ep_size, tp_size):
    shape = part.shape
    vmem = pl.BlockSpec(memory_space=pltpu.VMEM)
    return pl.pallas_call(
        functools.partial(router_kernel, (('ep', ep_size), ('tp', tp_size))),
        in_specs=[vmem],
        out_specs=vmem,
        out_shape=jax.ShapeDtypeStruct(shape, F32),
        scratch_shapes=[
            pltpu.VMEM((ep_size,) + shape, F32), pltpu.VMEM(shape, F32), pltpu.VMEM((tp_size,) + shape, F32),
            pltpu.SemaphoreType.DMA((ep_size,)), pltpu.SemaphoreType.DMA((ep_size,)),
            pltpu.SemaphoreType.DMA((tp_size,)), pltpu.SemaphoreType.DMA((tp_size,)),
        ],
        compiler_params=pltpu.CompilerParams(collective_id=3, has_side_effects=True),
        cost_estimate=pl.CostEstimate(flops=12 * part.size, bytes_accessed=8 * part.size, transcendentals=0),
        name="router_sum",
    )(part)


def solution(mesh):
    tp_size = mesh.shape['tp']
    ep_size = mesh.shape['ep']
    tok_spec = P(('dp', 'ep', 'tp'), None)
    in_w_spec = P('ep', None, 'tp')
    down_spec = P('ep', 'tp', None)
    out_w_spec = P(('dp', 'ep'), None, 'tp')
    out_down_spec = P(('dp', 'ep'), 'tp', None)

    def local_step(tokens, route_ids, w_router, w_gate, w_up, w_down, d_out):
        tok_loc, width = tokens.shape
        experts = w_router.shape[1]
        capacity = 4 * tok_loc // experts
        tok_all = lax.all_gather(tokens, ('ep', 'tp'), axis=0, tiled=False)
        dy_all = lax.all_gather(d_out, ('ep', 'tp'), axis=0, tiled=False)
        packed = [jnp.stack([w_gate[e], w_up[e], w_down[e]]) for e in range(w_gate.shape[0])]
        w_all = [lax.all_gather(w, 'tp', axis=0, tiled=False) for w in packed]

        gate_vals, slot_pos = route_local(tokens, route_ids, w_router)
        keys = (route_ids * KEY_STRIDE + slot_pos).astype(F32)
        meta = jnp.concatenate([keys.T, gate_vals.T], axis=0)
        meta_all = lax.all_gather(meta, ('ep', 'tp'), axis=0, tiled=False)

        pos = jnp.stack([lax.axis_index('ep'), lax.axis_index('tp'), jnp.int32(tp_size)]).astype(jnp.int32)
        grad_gate, grad_up, grad_down, xo, go = weight_grads(pos, tok_all, dy_all, meta_all, w_gate, w_up, w_down, capacity, tp_size)
        home0, home1 = [own_rows(xo, go, w_all[e], e, ep_size) for e in range(2)]
        cols = jnp.concatenate([keys, gate_vals, route_ids.astype(F32), jnp.zeros_like(gate_vals)], axis=1)
        block_out, grad_tokens, router_part = combine(home0, home1, cols, tokens, d_out, w_router.T)
        grad_router = router_sum(router_part, ep_size, tp_size).T
        return block_out, grad_tokens, grad_gate, grad_up, grad_down, grad_router

    return jax.shard_map(local_step, mesh=mesh, in_specs=(tok_spec, tok_spec, P(None, None), in_w_spec, in_w_spec, down_spec, tok_spec), out_specs=(tok_spec, tok_spec, out_w_spec, out_w_spec, out_down_spec, P('dp', None)), check_vma=False)
```

```python
import functools
import jax
import jax.numpy as jnp
from jax import lax
from jax.experimental import pallas as pl
from jax.experimental.pallas import tpu as pltpu
from jax.sharding import PartitionSpec as P

F32 = jnp.float32
BF16 = jnp.bfloat16
KEY_STRIDE = 4096
BLOCKS_PER_STEP = 2


def nn(a, b):
    return lax.dot_general(a, b, (((1,), (0,)), ((), ())), preferred_element_type=F32)


def nt(a, b):
    return lax.dot_general(a, b, (((1,), (1,)), ((), ())), preferred_element_type=F32)


def tn(a, b):
    return lax.dot_general(a, b, (((0,), (0,)), ((), ())), preferred_element_type=F32)


def hidden(h1, h3):
    sig = jax.nn.sigmoid(h1)
    return sig, (h1 * sig * h3).astype(BF16)


def hidden_back(da, h1, h3, sig):
    das = da * sig
    dz3 = (das * h1).astype(BF16)
    dz1 = (das * h3 * (1.0 + h1 * (1.0 - sig))).astype(BF16)
    return dz1, dz3


def route_local(tokens, route_ids, w_router):
    experts = w_router.shape[1]
    tok_loc = tokens.shape[0]
    expert_ids = jnp.arange(experts)
    logits = jnp.dot(tokens, w_router, preferred_element_type=F32)
    choice_hot = (route_ids[:, :, None] == expert_ids).astype(F32)
    chosen = jnp.sum(logits[:, None, :] * choice_hot, axis=2)
    gate_vals = jax.nn.softmax(chosen, axis=1)
    slot_order = (route_ids.T[:, :, None] == expert_ids).astype(jnp.int32).reshape(2 * tok_loc, experts)
    before = jnp.cumsum(slot_order, axis=0) - slot_order
    slot_pos = jnp.sum(before * slot_order, axis=1).reshape(2, tok_loc).T
    return gate_vals, slot_pos


def choose(pos_ref, meta_ref, b, e, e_loc):
    base = ((pos_ref[0] * e_loc + e) * KEY_STRIDE).astype(F32)
    k0 = meta_ref[b, 0:1, :] - base
    k1 = meta_ref[b, 1:2, :] - base
    use0 = jnp.logical_and(k0 >= 0.0, k0 < float(KEY_STRIDE))
    key = jnp.where(use0, k0, k1)
    gate = jnp.where(use0, meta_ref[b, 2:3, :], meta_ref[b, 3:4, :])
    return key, gate


def hidden_kernel(pos_ref, tok_ref, meta_ref, w1_ref, w3_ref, xs_ref, h1_ref, h3_ref):
    e_loc = w1_ref.shape[0]
    tok_loc = tok_ref.shape[1]
    cap = xs_ref.shape[2] // BLOCKS_PER_STEP
    slots = lax.broadcasted_iota(jnp.int32, (cap, tok_loc), 0).astype(F32)

    def per_expert(e, carry):
        for b in range(BLOCKS_PER_STEP):
            key, _ = choose(pos_ref, meta_ref, b, e, e_loc)
            sel = jnp.where(slots == key, 1.0, 0.0).astype(BF16)
            xs_ref[0, e, pl.ds(b * cap, cap), :] = nn(sel, tok_ref[b]).astype(BF16)
        x = xs_ref[0, e]
        h1_ref[0, e] = nn(x, w1_ref[e])
        h3_ref[0, e] = nn(x, w3_ref[e])
        return carry

    lax.fori_loop(0, e_loc, per_expert, 0)


def hidden_rows(pos, tok_all, meta_all, w1, w3, cap):
    blocks, tok_loc, width = tok_all.shape
    e_loc, _, cols = w1.shape
    steps = blocks // BLOCKS_PER_STEP
    rows = BLOCKS_PER_STEP * cap
    whole = lambda shape: pl.BlockSpec(shape, lambda i, p: (0,) * len(shape))
    out = lambda n: pl.BlockSpec((1, e_loc, rows, n), lambda i, p: (i, 0, 0, 0))
    return pl.pallas_call(
        hidden_kernel,
        grid_spec=pltpu.PrefetchScalarGridSpec(
            num_scalar_prefetch=1, grid=(steps,),
            in_specs=[pl.BlockSpec((BLOCKS_PER_STEP, tok_loc, width), lambda i, p: (i, 0, 0)),
                      pl.BlockSpec((BLOCKS_PER_STEP, meta_all.shape[1], tok_loc), lambda i, p: (i, 0, 0)),
                      whole(w1.shape), whole(w3.shape)],
            out_specs=[out(width), out(cols), out(cols)]),
        out_shape=[jax.ShapeDtypeStruct((steps, e_loc, rows, width), BF16),
                   jax.ShapeDtypeStruct((steps, e_loc, rows, cols), F32),
                   jax.ShapeDtypeStruct((steps, e_loc, rows, cols), F32)],
        compiler_params=pltpu.CompilerParams(dimension_semantics=("arbitrary",), vmem_limit_bytes=62 * 1024 * 1024),
        cost_estimate=pl.CostEstimate(flops=2 * blocks * e_loc * cap * (2 * width * cols + tok_loc * width),
                                      bytes_accessed=2 * tok_all.size + 8 * steps * e_loc * rows * cols, transcendentals=0),
        name="hidden_rows",
    )(pos, tok_all, meta_all, w1, w3)


def wgrad_kernel(pos_ref, dy_ref, meta_ref, xs_ref, h1_ref, h3_ref, w2_ref,
                 dw1_ref, dw3_ref, dw2_ref, xo_ref, go_ref, acc1, acc3, acc2, gs, az, z1, z3):
    step = pl.program_id(0)
    e_loc, cap = xo_ref.shape[1], xo_ref.shape[2]
    tok_loc = dy_ref.shape[1]
    cols = h1_ref.shape[3]
    chunk = 256

    @pl.when(step == 0)
    def _():
        acc1[...] = jnp.zeros_like(acc1)
        acc3[...] = jnp.zeros_like(acc3)
        acc2[...] = jnp.zeros_like(acc2)

    tp_size = pos_ref[2]
    slots = lax.broadcasted_iota(jnp.int32, (cap, tok_loc), 0).astype(F32)

    def per_expert(e, carry):
        for b in range(BLOCKS_PER_STEP):
            key, gate = choose(pos_ref, meta_ref, b, e, e_loc)
            hit = slots == key
            sel = jnp.where(hit, 1.0, 0.0).astype(BF16)
            g = jnp.sum(jnp.where(hit, gate, 0.0), axis=1, keepdims=True)
            gs[e, pl.ds(b * cap, cap), :] = (nn(sel, dy_ref[b]) * g).astype(BF16)
        x = xs_ref[0, e]
        dg = gs[e]
        for c in range(cols // chunk):
            cs = slice(c * chunk, (c + 1) * chunk)
            h1 = h1_ref[0, e, :, cs]
            h3 = h3_ref[0, e, :, cs]
            da = nt(dg, w2_ref[e, cs, :])
            sig, act = hidden(h1, h3)
            dz1, dz3 = hidden_back(da, h1, h3, sig)
            az[:, cs] = act
            z1[:, cs] = dz1
            z3[:, cs] = dz3
        acc1[e] += tn(x, z1[...])
        acc3[e] += tn(x, z3[...])
        acc2[e] += tn(az[...], dg)
        return carry

    lax.fori_loop(0, e_loc, per_expert, 0)

    per_group = tp_size // BLOCKS_PER_STEP
    mine = pos_ref[1]

    @pl.when(lax.rem(step, per_group) == mine // BLOCKS_PER_STEP)
    def _():
        rows = pl.ds(pl.multiple_of(lax.rem(mine, BLOCKS_PER_STEP) * cap, cap), cap)
        xo_ref[0] = xs_ref[0, :, rows, :]
        go_ref[0] = gs[:, rows, :]

    @pl.when(step == pl.num_programs(0) - 1)
    def _():
        dw1_ref[...] = acc1[...].astype(BF16)
        dw3_ref[...] = acc3[...].astype(BF16)
        dw2_ref[...] = acc2[...].astype(BF16)


def weight_grads(pos, dy_all, meta_all, xs, h1, h3, w1, w3, w2, cap, tp_size):
    blocks, tok_loc, width = dy_all.shape
    e_loc, _, cols = w1.shape
    steps = blocks // BLOCKS_PER_STEP
    per_group = tp_size // BLOCKS_PER_STEP
    rows = BLOCKS_PER_STEP * cap
    whole = lambda shape, **kw: pl.BlockSpec(shape, lambda i, p: (0,) * len(shape), **kw)
    own = pl.BlockSpec((1, e_loc, cap, width), lambda i, p: (i // per_group, 0, 0, 0))
    tile = lambda a: pl.BlockSpec((1,) + a.shape[1:], lambda i, p: (i, 0, 0, 0))
    grid_spec = pltpu.PrefetchScalarGridSpec(
        num_scalar_prefetch=1,
        grid=(steps,),
        in_specs=[
            pl.BlockSpec((BLOCKS_PER_STEP, tok_loc, width), lambda i, p: (i, 0, 0)),
            pl.BlockSpec((BLOCKS_PER_STEP, meta_all.shape[1], tok_loc), lambda i, p: (i, 0, 0)),
            tile(xs), tile(h1), tile(h3), whole(w2.shape, pipeline_mode=pl.Buffered(1)),
        ],
        out_specs=[whole(w1.shape), whole(w3.shape), whole(w2.shape), own, own],
        scratch_shapes=[
            pltpu.VMEM(w1.shape, F32), pltpu.VMEM(w3.shape, F32), pltpu.VMEM(w2.shape, F32),
            pltpu.VMEM((e_loc, rows, width), BF16),
            pltpu.VMEM((rows, cols), BF16), pltpu.VMEM((rows, cols), BF16), pltpu.VMEM((rows, cols), BF16),
        ],
    )
    own_shape = jax.ShapeDtypeStruct((blocks // tp_size, e_loc, cap, width), BF16)
    flops = 2 * blocks * e_loc * cap * (4 * width * cols + tok_loc * width)
    return pl.pallas_call(
        wgrad_kernel,
        grid_spec=grid_spec,
        out_shape=[jax.ShapeDtypeStruct(w.shape, BF16) for w in (w1, w3, w2)] + [own_shape, own_shape],
        compiler_params=pltpu.CompilerParams(dimension_semantics=("arbitrary",), vmem_limit_bytes=63 * 1024 * 1024),
        cost_estimate=pl.CostEstimate(flops=flops, bytes_accessed=2 * dy_all.size + 8 * h1.size, transcendentals=0),
        name="weight_grads",
    )(pos, dy_all, meta_all, xs, h1, h3, w2)


def ep_peers(ep_size, me):
    return [lax.rem(me + k, ep_size) for k in range(1, ep_size)]


def rows_kernel(ep_size, tile, x_ref, g_ref, w_hbm, home_ref, o_acc, q_acc, w_ref, send, relay,
                w_sem, send_sem, recv_sem, relay_send, relay_recv, forward_sem, self_sem):
    step = pl.program_id(0)
    steps = ep_size // tile
    me = lax.axis_index('ep')
    chip = me // tile
    mine = lax.rem(me, tile)
    cap, width = x_ref.shape[2], x_ref.shape[3]

    def weights(j):
        return pltpu.make_async_copy(w_hbm.at[j], w_ref.at[j], w_sem.at[j])

    @pl.when(step == 0)
    def _():
        for j in range(w_ref.shape[0]):
            weights(j).start()
        barrier = pltpu.get_barrier_semaphore()
        for peer in ep_peers(ep_size, me):
            pl.semaphore_signal(barrier, inc=1, device_id={'ep': peer}, device_id_type=pl.DeviceIdType.MESH)
        pl.semaphore_wait(barrier, ep_size - 1)

    def hop(at):
        return (2 + 3 * at + 3 * (at // 2) + 2 * (at // 3)) % 4

    def chip_at(offset):
        return lax.rem(chip + offset, steps) * tile

    def push(src, dst, send_at, recv_at, dest):
        return pltpu.make_async_remote_copy(
            src_ref=src, dst_ref=dst, send_sem=send_at, recv_sem=recv_at,
            device_id={'ep': dest}, device_id_type=pl.DeviceIdType.MESH)

    def direct(slot, src_dev, dest):
        return push(send.at[slot], home_ref.at[src_dev], send_sem.at[slot], recv_sem.at[src_dev, 0], dest)

    def via(part, c):
        near = chip_at(1 if part == 0 else steps - 1) + mine
        return push(send.at[c, part], relay.at[part, c], relay_send.at[part, c], relay_recv.at[part, c], near)

    def forward(part, c):
        source = chip_at(steps - 1 if part == 0 else 1) + mine
        dest = chip_at(1 if part == 0 else steps - 1) + c
        return push(relay.at[part, c], home_ref.at[source, part], forward_sem.at[part, c], recv_sem.at[source, part], dest)

    @pl.when(step == 1)
    def _():
        for c in range(tile):
            for part in range(2):
                via(part, c).start()

    @pl.when(step == 2)
    def _():
        for c in range(tile):
            for part in range(2):
                via(part, c).wait_recv()
                forward(part, c).start()

    for at in (1, 2):
        @pl.when(step == at + 1)
        def _(at=at):
            for c in range(tile):
                direct(at * tile + c, me, chip_at(hop(at)) + c).start()

    dest = lax.rem(chip + (2 + 3 * step + 3 * (step // 2) + 2 * (step // 3)), steps) * tile
    x = x_ref[pl.ds(dest, tile), 0].reshape(tile * cap, width)
    dg = g_ref[pl.ds(dest, tile), 0].reshape(tile * cap, width)
    o_acc[...] = jnp.zeros_like(o_acc)
    q_acc[...] = jnp.zeros_like(q_acc)

    def part(j, carry):
        @pl.when(step == 0)
        def _():
            weights(j).wait()

        w1 = w_ref[j, 0]
        w3 = w_ref[j, 1]
        w2 = w_ref[j, 2]
        h1 = nn(x, w1)
        h3 = nn(x, w3)
        da = nt(dg, w2)
        sig, act = hidden(h1, h3)
        dz1, dz3 = hidden_back(da, h1, h3, sig)
        o_acc[...] += nn(act, w2).astype(BF16).astype(F32)
        q_acc[...] += (nt(dz1, w1) + nt(dz3, w3)).astype(BF16).astype(F32)
        return carry

    lax.fori_loop(0, w_ref.shape[0], part, 0)
    for c in range(tile):
        rows = slice(c * cap, (c + 1) * cap)
        send[step * tile + c, 0] = o_acc[rows].astype(BF16)
        send[step * tile + c, 1] = q_acc[rows].astype(BF16)

    @pl.when(step == steps - 1)
    def _():
        last = (steps - 1) * tile
        own = pltpu.make_async_copy(send.at[last + mine], home_ref.at[me], self_sem)
        own.start()
        near = chip * tile
        for k in range(1, tile):
            c = lax.rem(mine + k, tile)
            direct(last + c, me, near + c).start()
        for c in range(tile):
            for part in range(2):
                via(part, c).wait_send()
                forward(part, c).wait_send()
        for slot in range(tile, last):
            direct(slot, me, me).wait_send()
        for k in range(1, tile):
            direct(last + lax.rem(mine + k, tile), me, me).wait_send()
        for offset in range(steps):
            for k in range(tile):
                if offset == 0 and k == 0:
                    continue
                peer = chip_at(offset) + lax.rem(mine + k, tile)
                if offset == 2:
                    for part in range(2):
                        push(relay.at[part, 0], home_ref.at[peer, part], forward_sem.at[part, 0], recv_sem.at[peer, part], peer).wait_recv()
                else:
                    direct(0, peer, peer).wait_recv()
        own.wait()


def own_rows(xo, go, wg, e, ep_size):
    groups, e_loc, cap, width = xo.shape
    tp_size, _, _, cols = wg.shape
    tile = 2
    in_rows = pl.BlockSpec((groups, 1, cap, width), lambda r: (0, e, 0, 0))
    flops = 12 * groups * cap * width * cols * tp_size
    return pl.pallas_call(
        functools.partial(rows_kernel, ep_size, tile),
        grid=(groups // tile,),
        in_specs=[in_rows, in_rows, pl.BlockSpec(memory_space=pl.ANY)],
        out_specs=pl.BlockSpec(memory_space=pl.ANY),
        out_shape=jax.ShapeDtypeStruct((groups, 2, cap, width), BF16),
        scratch_shapes=[
            pltpu.VMEM((tile * cap, width), F32), pltpu.VMEM((tile * cap, width), F32),
            pltpu.VMEM(wg.shape, BF16),
            pltpu.VMEM((groups, 2, cap, width), BF16),
            pltpu.VMEM((2, tile, cap, width), BF16),
            pltpu.SemaphoreType.DMA((tp_size,)),
            pltpu.SemaphoreType.DMA((groups,)), pltpu.SemaphoreType.DMA((groups, 2)),
            pltpu.SemaphoreType.DMA((2, tile)), pltpu.SemaphoreType.DMA((2, tile)), pltpu.SemaphoreType.DMA((2, tile)),
            pltpu.SemaphoreType.DMA,
        ],
        compiler_params=pltpu.CompilerParams(dimension_semantics=("arbitrary",), vmem_limit_bytes=62 * 1024 * 1024,
                                             collective_id=1 + e, has_side_effects=True),
        cost_estimate=pl.CostEstimate(flops=flops, bytes_accessed=4 * xo.size + 2 * wg.size, transcendentals=0),
        name="own_rows",
    )(xo, go, wg)


def combine_kernel(home0_ref, home1_ref, col_ref, tok_ref, dy_ref, wr_ref, y_ref, du_ref, dwr_ref, p0, p1, px):
    step = pl.program_id(0)
    cap = home0_ref.shape[2]
    tok_loc = tok_ref.shape[0]
    experts = wr_ref.shape[0]

    lane = lax.broadcasted_iota(jnp.int32, (1, 2 * cap), 1)
    target = (step * 2 * KEY_STRIDE + jnp.where(lane >= cap, lane + (KEY_STRIDE - cap), lane)).astype(F32)
    hit0 = col_ref[:, 0:1] == target
    hit1 = col_ref[:, 1:2] == target
    s0 = jnp.where(hit0, 1.0, 0.0).astype(BF16)
    s1 = jnp.where(hit1, 1.0, 0.0).astype(BF16)
    rows_o = jnp.concatenate([home0_ref[0, 0], home1_ref[0, 0]], axis=0)
    rows_x = jnp.concatenate([home0_ref[0, 1], home1_ref[0, 1]], axis=0)

    @pl.when(step == 0)
    def _():
        p0[...] = nn(s0, rows_o)
        p1[...] = nn(s1, rows_o)
        px[...] = nn(s0 + s1, rows_x)

    @pl.when(step > 0)
    def _():
        p0[...] += nn(s0, rows_o)
        p1[...] += nn(s1, rows_o)
        px[...] += nn(s0 + s1, rows_x)

    @pl.when(step == pl.num_programs(0) - 1)
    def _():
        g0 = col_ref[:, 2:3]
        g1 = col_ref[:, 3:4]
        dy = dy_ref[...].astype(F32)
        a0 = p0[...]
        a1 = p1[...]
        y_ref[...] = (g0 * a0 + g1 * a1).astype(BF16)
        d0 = jnp.sum(a0 * dy, axis=1, keepdims=True)
        d1 = jnp.sum(a1 * dy, axis=1, keepdims=True)
        mean = g0 * d0 + g1 * d1
        ids = lax.broadcasted_iota(jnp.int32, (tok_loc, experts), 1).astype(F32)
        dlog = (jnp.where(col_ref[:, 4:5] == ids, g0 * (d0 - mean), 0.0)
                + jnp.where(col_ref[:, 5:6] == ids, g1 * (d1 - mean), 0.0)).astype(BF16)
        du_ref[...] = (px[...] + nn(dlog, wr_ref[...])).astype(BF16)
        dwr_ref[...] = tn(dlog, tok_ref[...])


def combine(home0, home1, cols, tokens, d_out, wr_t):
    groups, _, cap, width = home0.shape
    tok_loc = tokens.shape[0]
    experts = wr_t.shape[0]
    home = pl.BlockSpec((1, 2, cap, width), lambda s: (s, 0, 0, 0))
    whole = lambda a: pl.BlockSpec(a.shape, lambda s: (0,) * a.ndim)
    return pl.pallas_call(
        combine_kernel,
        grid=(groups,),
        in_specs=[home, home, whole(cols), whole(tokens), whole(d_out), whole(wr_t)],
        out_specs=[whole(tokens), whole(tokens), pl.BlockSpec((experts, width), lambda s: (0, 0))],
        out_shape=[jax.ShapeDtypeStruct(tokens.shape, BF16), jax.ShapeDtypeStruct(tokens.shape, BF16),
                   jax.ShapeDtypeStruct((experts, width), F32)],
        scratch_shapes=[pltpu.VMEM(tokens.shape, F32)] * 3,
        compiler_params=pltpu.CompilerParams(dimension_semantics=("arbitrary",), vmem_limit_bytes=62 * 1024 * 1024),
        cost_estimate=pl.CostEstimate(flops=6 * tok_loc * experts * cap * width, bytes_accessed=4 * home0.size, transcendentals=0),
        name="combine",
    )(home0, home1, cols, tokens, d_out, wr_t)


def router_kernel(axes, part_ref, out_ref, buf_a, mid, buf_b, send_a, recv_a, send_b, recv_b):
    sizes = [size for _, size in axes]
    barrier = pltpu.get_barrier_semaphore()
    for name, size in axes:
        me = lax.axis_index(name)
        for k in range(1, size):
            pl.semaphore_signal(barrier, inc=1, device_id={name: lax.rem(me + k, size)}, device_id_type=pl.DeviceIdType.MESH)
    pl.semaphore_wait(barrier, sum(sizes) - len(sizes))

    def exchange(name, size, src, buf, send_sem, recv_sem, out):
        me = lax.axis_index(name)
        copies = []
        for k in range(1, size):
            copy = pltpu.make_async_remote_copy(
                src_ref=src, dst_ref=buf.at[me], send_sem=send_sem.at[k], recv_sem=recv_sem.at[me],
                device_id={name: lax.rem(me + k, size)}, device_id_type=pl.DeviceIdType.MESH)
            copy.start()
            copies.append(copy)
        buf[me] = src[...]
        for k in range(1, size):
            peer = lax.rem(me + k, size)
            pltpu.make_async_remote_copy(
                src_ref=src, dst_ref=buf.at[peer], send_sem=send_sem.at[k], recv_sem=recv_sem.at[peer],
                device_id={name: peer}, device_id_type=pl.DeviceIdType.MESH).wait_recv()
        total = buf[0]
        for k in range(1, size):
            total = total + buf[k]
        out[...] = total
        return copies

    copies = exchange(*axes[0], part_ref, buf_a, send_a, recv_a, mid)
    copies += exchange(*axes[1], mid, buf_b, send_b, recv_b, out_ref)
    for copy in copies:
        copy.wait_send()


def router_sum(part, ep_size, tp_size):
    shape = part.shape
    vmem = pl.BlockSpec(memory_space=pltpu.VMEM)
    return pl.pallas_call(
        functools.partial(router_kernel, (('ep', ep_size), ('tp', tp_size))),
        in_specs=[vmem],
        out_specs=vmem,
        out_shape=jax.ShapeDtypeStruct(shape, F32),
        scratch_shapes=[
            pltpu.VMEM((ep_size,) + shape, F32), pltpu.VMEM(shape, F32), pltpu.VMEM((tp_size,) + shape, F32),
            pltpu.SemaphoreType.DMA((ep_size,)), pltpu.SemaphoreType.DMA((ep_size,)),
            pltpu.SemaphoreType.DMA((tp_size,)), pltpu.SemaphoreType.DMA((tp_size,)),
        ],
        compiler_params=pltpu.CompilerParams(collective_id=3, has_side_effects=True),
        cost_estimate=pl.CostEstimate(flops=12 * part.size, bytes_accessed=8 * part.size, transcendentals=0),
        name="router_sum",
    )(part)


def solution(mesh):
    tp_size = mesh.shape['tp']
    ep_size = mesh.shape['ep']
    tok_spec = P(('dp', 'ep', 'tp'), None)
    in_w_spec = P('ep', None, 'tp')
    down_spec = P('ep', 'tp', None)
    out_w_spec = P(('dp', 'ep'), None, 'tp')
    out_down_spec = P(('dp', 'ep'), 'tp', None)

    def local_step(tokens, route_ids, w_router, w_gate, w_up, w_down, d_out):
        tok_loc, width = tokens.shape
        experts = w_router.shape[1]
        capacity = 4 * tok_loc // experts
        tok_all = lax.all_gather(tokens, ('ep', 'tp'), axis=0, tiled=False)
        dy_all = lax.all_gather(d_out, ('ep', 'tp'), axis=0, tiled=False)
        packed = [jnp.stack([w_gate[e], w_up[e], w_down[e]]) for e in range(w_gate.shape[0])]
        w_all = [lax.all_gather(w, 'tp', axis=0, tiled=False) for w in packed]

        gate_vals, slot_pos = route_local(tokens, route_ids, w_router)
        keys = (route_ids * KEY_STRIDE + slot_pos).astype(F32)
        meta = jnp.concatenate([keys.T, gate_vals.T], axis=0)
        meta_all = lax.all_gather(meta, ('ep', 'tp'), axis=0, tiled=False)

        pos = jnp.stack([lax.axis_index('ep'), lax.axis_index('tp'), jnp.int32(tp_size)]).astype(jnp.int32)
        xs, h1, h3 = hidden_rows(pos, tok_all, meta_all, w_gate, w_up, capacity)
        grad_gate, grad_up, grad_down, xo, go = weight_grads(pos, dy_all, meta_all, xs, h1, h3, w_gate, w_up, w_down, capacity, tp_size)
        home0, home1 = [own_rows(xo, go, w_all[e], e, ep_size) for e in range(2)]
        cols = jnp.concatenate([keys, gate_vals, route_ids.astype(F32), jnp.zeros_like(gate_vals)], axis=1)
        block_out, grad_tokens, router_part = combine(home0, home1, cols, tokens, d_out, w_router.T)
        grad_router = router_sum(router_part, ep_size, tp_size).T
        return block_out, grad_tokens, grad_gate, grad_up, grad_down, grad_router

    return jax.shard_map(local_step, mesh=mesh, in_specs=(tok_spec, tok_spec, P(None, None), in_w_spec, in_w_spec, down_spec, tok_spec), out_specs=(tok_spec, tok_spec, out_w_spec, out_w_spec, out_down_spec, P('dp', None)), check_vma=False)
```
